32 devices in a mesh: dp: 4 (over y, x), ctx: 8 (over z, core).
Axes of the slice: x: 2, y: 2, z: 4, core: 2. Of those that a mesh axis runs over, the one named last changes fastest.
Arguments:
- queries: bfloat16 [4096, 4096], P(('dp', 'ctx')), parts along dimension 0, may hold values from -9 to 9
- keys: bfloat16 [4096, 512], P(('dp', 'ctx')), parts along dimension 0, may hold values from -9 to 9
- values: bfloat16 [4096, 512], P(('dp', 'ctx')), parts along dimension 0, may hold values from -6 to 6
- doc_lengths: int32 [32], P('dp'), parts along dimension 0, may hold values from 1 to 512, as said below
- row_owner: int32 [4096, 1], P(('dp', 'ctx')), parts along dimension 0, may hold values from 0 to 7; in each aligned block of 128 rows (0 to 127, 128 to 255, ...) at most 24 rows name the same one
Outputs:
- handed: bfloat16 [6144, 4096], P(('dp', 'ctx')), parts along dimension 0
The draws below stay inside these ranges and needn't reach their ends.
There are 4 independent parts, one for each index of `dp`. The reference program is written for one: setup_inputs(seed, part) draws one part's arguments, and reference() takes and returns one part's arrays. A program takes and returns all parts, laid end to end along the dimension named above; each array names one. Nothing has to cross between parts.
Inputs may be any that keep to these rules, and one draw needn't show every extreme that they name: `doc_lengths`: the lengths sum to 1024; the longest is exactly 512. `row_owner`: among the 128 rows of one device, no owner is named more than 24 times.
All inputs are finite; a program needn't handle non-finite values.
Results may differ from the reference program's by a relative error of at most 0.0046.
Values may be sent and summed in bfloat16 or wider, within the bound.
No kernel may reach another device: no remote copies, remote signals or barrier semaphores. Data moves between devices by JAX's collectives and lax.ppermute only.
A program may use at most 64 MiB of HBM per device.

```python
import math
import jax
import jax.numpy as jnp
import numpy as np
from jax import lax

HEADS = 32
KVH = 4
HD = 128
TOK_DEV = 128
WIN_DEV = 4
MAXDOC = 512
TOKENS = 1024
DOCS = 8
MOST = 24
N_CTX = 8


def draw_queries(key, part):
    base = jnp.clip(jax.random.normal(jax.random.fold_in(key, 1), (TOKENS, HEADS * HD), jnp.float32), -4.0, 4.0)
    return base.astype(jnp.bfloat16)


def draw_keys(key, part):
    base = jnp.clip(jax.random.normal(jax.random.fold_in(key, 2), (TOKENS, KVH * HD), jnp.float32), -4.0, 4.0)
    return base.astype(jnp.bfloat16)


def draw_doc_lengths(key, part):
    leading = DOCS - 2
    lead_total = (N_CTX - WIN_DEV) * TOK_DEV - TOK_DEV // 2
    jitter_span = max((lead_total // leading - 2) // 2, 0)
    steps_index = jnp.arange(1, leading, dtype=jnp.int32)
    jitter = jax.random.randint(jax.random.fold_in(key, 11), (leading - 1,), -jitter_span, jitter_span + 1, dtype=jnp.int32)
    cuts = steps_index * lead_total // leading + jitter
    edges = jnp.concatenate([jnp.zeros((1,), jnp.int32), cuts, jnp.full((1,), lead_total, jnp.int32)])
    parts_lengths = edges[1:] - edges[:-1]
    tail = jnp.array([MAXDOC, TOK_DEV // 2], jnp.int32)
    return jnp.concatenate([parts_lengths, tail]).astype(jnp.int32)


def block_levels(stream_key, extent, split, least, top_value):
    gain, own = 1.0, jax.random.fold_in(stream_key, 6)
    for axis_at, shards_of in split:
        heights = jnp.exp(jax.random.uniform(jax.random.fold_in(own, axis_at), (shards_of,), jnp.float32, least / len(split), top_value / len(split)))
        gain = gain * jnp.repeat(heights, extent[axis_at] // shards_of).reshape([-1 if axis == axis_at else 1 for axis in range(len(extent))])
    return gain


def routed_block(rng, own, number, rows, count, top, reach, slope):
    ranking = jax.random.permutation(rng, count)
    crowded, usual = load_shares(count, rows * top, reach, slope, True), load_shares(count, rows * top, reach, slope, False)
    places = jnp.arange(count)

    def named(lengths, offset_by):
        used = int((lengths > 0).sum())
        fixed = max(1, used // 4)
        passed = fixed + (places - fixed + offset_by * (used - fixed)) % max(1, count - fixed)
        return jnp.zeros((count,), jnp.int32).at[ranking[jnp.where(places < fixed, places, passed)]].set(jnp.asarray(lengths, jnp.int32))

    lengths = jnp.where(number % 4 == 0, named(crowded, number // 4), named(usual, number - number // 4 - 1))
    mixed = jax.random.permutation(jax.random.fold_in(own, 3), count)
    source_of, sink = mixed[0:count // 2 * 2:2], mixed[1:count // 2 * 2:2]
    slack = jnp.minimum(lengths[source_of] - 1, reach - lengths[sink]) // 2
    slack = jnp.where((source_of == ranking[0]) | (sink == ranking[0]) | (lengths[sink] == 0), 0, jnp.maximum(slack, 0))
    passed = jax.random.randint(jax.random.fold_in(own, 4), (count // 2,), 0, 1 << 20) % (slack + 1)
    lengths = lengths.at[source_of].add(-passed).at[sink].add(passed)
    labels = jnp.searchsorted(jnp.cumsum(lengths), jnp.arange(rows * top), side="right").astype(jnp.int32)
    listing = labels.reshape(top, rows).T
    listing = listing[jax.random.permutation(jax.random.fold_in(own, 1), rows)]
    offset_by = jax.random.randint(jax.random.fold_in(own, 2), (rows, 1), 0, top)
    return jnp.take_along_axis(listing, (jnp.arange(top)[None, :] + offset_by) % top, axis=1)


def load_shares(number_of, total, reach, slope, full):
    portions = [(1 << 20) // math.isqrt(grade ** slope) + 1 for grade in range(1, number_of + 1)]
    largest = reach if full else min(reach, max(-(-total // number_of), total * portions[0] // sum(portions)))
    least = 1 if total - largest >= number_of - 1 else 0
    given, spare = [largest] + [least] * (number_of - 1), total - largest - least * (number_of - 1)
    while spare > 0:
        candidates = [i for i in range(1, number_of) if given[i] < largest] or [i for i in range(1, number_of) if given[i] < reach]
        whole, left = sum([portions[i] for i in candidates]), spare
        for i in candidates:
            more = min(reach - given[i], max(1, left * portions[i] // whole), spare)
            given[i] = given[i] + more
            spare = spare - more
    return np.array(given)


def centred(stream_key, extent, width, limit, pieces=(), held_as=jnp.bfloat16):
    drawn = jax.random.normal(stream_key, extent, jnp.float32) * width
    if len(pieces) > 0:
        drawn = block_levels(stream_key, extent, pieces, -0.22, 0.18) * drawn
    return jnp.clip(drawn, min=-limit, max=limit).astype(held_as)


def setup_inputs(seed: int = 0, part: int = 0) -> dict:
    splits = jax.random.split(jax.random.key(seed), 6)
    own_keys = jax.random.split(jax.random.fold_in(splits[5], part), 6)
    queries = draw_queries(jax.random.fold_in(jax.random.fold_in(splits[5], part), 71), part)
    keys = draw_keys(jax.random.fold_in(jax.random.fold_in(splits[5], part), 71), part)
    values = centred(own_keys[2], (TOKENS, KVH * HD), 1.0, 6.0, ((0, 8),))
    doc_lengths = draw_doc_lengths(jax.random.fold_in(jax.random.fold_in(splits[5], part), 71), part)
    row_owner_keys = jax.random.split(jax.random.fold_in(own_keys[4], 1), TOKENS // TOK_DEV)
    row_owner_turns = jax.random.permutation(jax.random.fold_in(own_keys[4], 3), TOKENS // TOK_DEV)
    row_owner = jax.vmap(lambda own, number: routed_block(jax.random.fold_in(own_keys[4], 2), own, number, TOK_DEV, N_CTX, 1, MOST, 2))(row_owner_keys, row_owner_turns).reshape((TOKENS, 1))
    return {"queries": queries, "keys": keys, "values": values, "doc_lengths": doc_lengths, "row_owner": row_owner}


masked_score = -1e+30

def doc_numbers(doc_lengths, positions):
    doc_ends = jnp.cumsum(doc_lengths)
    return lax.optimization_barrier(jnp.sum((doc_ends[None, :] <= positions[:, None]).astype(jnp.int32), axis=1))

def attend_block(query_block, key_window, value_window, query_pos, key_pos, doc_lengths):
    row_count = query_block.shape[0]
    group_size = HEADS // KVH
    grouped = query_block.astype(jnp.float32).reshape(row_count, KVH, group_size, HD)
    key_heads = key_window.astype(jnp.float32).reshape(-1, KVH, HD)
    value_heads = value_window.astype(jnp.float32).reshape(-1, KVH, HD)
    scores = jnp.einsum('tkgd,skd->kgts', grouped, key_heads) * (1.0 / math.sqrt(HD))
    query_doc = doc_numbers(doc_lengths, query_pos)
    key_doc = doc_numbers(doc_lengths, key_pos)
    allowed = (query_doc[:, None] == key_doc[None, :]) & (key_pos[None, :] <= query_pos[:, None]) & (key_pos[None, :] >= 0)
    scores = jnp.where(allowed[None, None], scores, masked_score)
    peak = lax.optimization_barrier(jnp.max(scores, axis=-1, keepdims=True))
    weights = jnp.exp(scores - peak)
    total = lax.optimization_barrier(jnp.sum(weights, axis=-1, keepdims=True))
    probs = (weights / total).astype(jnp.bfloat16)
    mixed = jnp.einsum('kgts,skd->tkgd', probs.astype(jnp.float32), value_heads)
    return mixed.reshape(row_count, HEADS * HD).astype(jnp.bfloat16)

def reference(queries, keys, values, doc_lengths, row_owner):
    reach_rows = WIN_DEV * TOK_DEV
    padded_keys = jnp.concatenate([jnp.zeros((reach_rows, keys.shape[1]), keys.dtype), keys], axis=0)
    padded_values = jnp.concatenate([jnp.zeros((reach_rows, values.shape[1]), values.dtype), values], axis=0)

    def one_block(block_number):
        start = (block_number * TOK_DEV).astype(jnp.int32)
        query_block = lax.dynamic_slice_in_dim(queries, start, TOK_DEV, 0)
        key_window = lax.dynamic_slice_in_dim(padded_keys, start, reach_rows + TOK_DEV, 0)
        value_window = lax.dynamic_slice_in_dim(padded_values, start, reach_rows + TOK_DEV, 0)
        query_pos = start + jnp.arange(TOK_DEV, dtype=jnp.int32)
        key_pos = start - reach_rows + jnp.arange(reach_rows + TOK_DEV, dtype=jnp.int32)
        return attend_block(query_block, key_window, value_window, query_pos, key_pos, doc_lengths)
    attended = lax.map(one_block, jnp.arange(N_CTX, dtype=jnp.int32)).reshape(TOKENS, HEADS * HD)
    owners = row_owner[:, 0].reshape(N_CTX, TOK_DEV)
    onehot = (owners[:, :, None] == jnp.arange(N_CTX, dtype=jnp.int32)[None, None, :]).astype(jnp.int32)
    earlier = jnp.cumsum(onehot, axis=1) - onehot
    rank = lax.optimization_barrier(jnp.sum(earlier * onehot, axis=2))
    source = jnp.arange(N_CTX, dtype=jnp.int32)[:, None]
    target = ((owners * N_CTX + source) * MOST + rank).reshape(TOKENS).astype(jnp.int32)
    handed = jnp.zeros((N_CTX * N_CTX * MOST, HEADS * HD), jnp.bfloat16).at[target].set(attended)
    return handed
```

```python
import functools
import math

import jax
import jax.numpy as jnp
from jax import lax
from jax.experimental import pallas as pl
from jax.experimental.pallas import tpu as pltpu
from jax.sharding import PartitionSpec as P

HEADS = 32
KVH = 4
HD = 128
WIN_DEV = 4

masked_score = -1e30


def shifted(block, axis, distance):
    devices = range(lax.axis_size(axis))
    route = [(i - distance, i) for i in devices if i - distance in devices]
    return lax.ppermute(block, axis, route)


def block_scores(grouped, key_part, allowed_part):
    key_heads = key_part.reshape(key_part.shape[0], grouped.shape[1], HD)
    scores = jnp.einsum(
        "tkgd,skd->kgts", grouped, key_heads, preferred_element_type=jnp.float32
    ) * (1.0 / math.sqrt(HD))
    return jnp.where(allowed_part[None, None], scores, masked_score)


def softmax_weights(scores):
    peak = jnp.max(scores, axis=-1, keepdims=True)
    weights = jnp.exp(scores - peak)
    total = jnp.sum(weights, axis=-1, keepdims=True)
    return (weights / total).astype(jnp.bfloat16)


def mix_block(probs_part, value_part):
    value_heads = value_part.reshape(value_part.shape[0], probs_part.shape[0], HD)
    return jnp.einsum("kgts,skd->tkgd", probs_part, value_heads, preferred_element_type=jnp.float32)


def doc_numbers(doc_ends, positions):
    return jnp.sum((doc_ends[None, :] <= positions[:, None]).astype(jnp.int32), axis=1)


def plain_body(queries, keys, values, doc_lengths, row_owner, slot_count):
    row_count = queries.shape[0]
    ctx_count = lax.axis_size("ctx")
    device_index = lax.axis_index("ctx")
    group_size = HEADS // KVH
    stack_keys, stack_values = (keys, values)
    reach_width = 1
    for _ in range(WIN_DEV.bit_length() - 1):
        moved_keys, moved_values = shifted((stack_keys, stack_values), "ctx", reach_width)
        stack_keys = jnp.concatenate([moved_keys, stack_keys], axis=0)
        stack_values = jnp.concatenate([moved_values, stack_values], axis=0)
        reach_width = reach_width * 2
    far_keys, far_values = shifted((keys, values), "ctx", WIN_DEV)
    window_keys = jnp.concatenate([far_keys, stack_keys], axis=0)
    window_values = jnp.concatenate([far_values, stack_values], axis=0)
    query_pos = device_index * row_count + lax.iota(jnp.int32, row_count)
    key_pos = (device_index - WIN_DEV) * row_count + lax.iota(jnp.int32, (WIN_DEV + 1) * row_count)
    doc_ends = jnp.cumsum(doc_lengths)
    query_doc = doc_numbers(doc_ends, query_pos)
    key_doc = doc_numbers(doc_ends, key_pos)
    allowed = (
        (query_doc[:, None] == key_doc[None, :])
        & (key_pos[None, :] <= query_pos[:, None])
        & (key_pos[None, :] >= 0)
    )
    grouped_all = queries.reshape(row_count, KVH, group_size, HD)
    owner_column = row_owner[:, 0]
    onehot = (owner_column[:, None] == lax.iota(jnp.int32, ctx_count)[None, :]).astype(jnp.int32)
    earlier_count = jnp.cumsum(onehot, axis=0) - onehot
    slot_rank = jnp.sum(earlier_count * onehot, axis=1)
    slot_index = owner_column * slot_count + slot_rank
    probs = softmax_weights(block_scores(grouped_all, window_keys, allowed))
    attended = mix_block(probs, window_values)
    merged = attended.reshape(row_count, HEADS * HD).astype(jnp.bfloat16)
    return lax.all_to_all(
        jnp.zeros((ctx_count * slot_count, merged.shape[1]), jnp.bfloat16)
        .at[slot_index]
        .set(merged),
        "ctx",
        split_axis=0,
        concat_axis=0,
        tiled=True,
    )


VM = pltpu.VMEM
INFO = 128
GRANT = 16 * 1024 * 1024


def order_kernel(ctx_count, slot_count, me_ref, doc_ref, owner_ref, q_ref, qs_ref, info_ref):
    rows = owner_ref.shape[1]
    slots = ctx_count * slot_count
    owner = owner_ref[...]
    onehot = (lax.broadcasted_iota(jnp.int32, (ctx_count, rows), 0) == owner).astype(jnp.float32)
    upper = (
        lax.broadcasted_iota(jnp.int32, (rows, rows), 0)
        < lax.broadcasted_iota(jnp.int32, (rows, rows), 1)
    ).astype(jnp.bfloat16)
    count = jnp.dot(onehot.astype(jnp.bfloat16), upper, preferred_element_type=jnp.float32)
    rank = jnp.sum(count * onehot, axis=0, keepdims=True).astype(jnp.int32)
    target = owner * slot_count + rank
    pick = lax.broadcasted_iota(jnp.int32, (slots, rows), 0) == target
    place = lax.broadcasted_iota(jnp.int32, (slots, rows), 1)
    row_of = jnp.max(jnp.where(pick, place, -1), axis=1, keepdims=True)
    filled = row_of >= 0
    pos = row_of + me_ref[0] * rows
    start = jnp.zeros_like(pos)
    end = jnp.int32(0)
    for c in range(doc_ref.shape[0]):
        end = end + doc_ref[c]
        start = jnp.where(end <= pos, jnp.maximum(start, end), start)
    hi = jnp.where(filled, pos, -1)
    lane = lax.broadcasted_iota(jnp.int32, (slots, INFO), 1)
    info_ref[...] = jnp.where(lane == 0, start, hi)
    pick = jnp.where(pick, 1.0, 0.0).astype(jnp.bfloat16)
    for h in range(HEADS):
        qs_ref[h] = jnp.dot(
            pick, q_ref[:, h * HD : (h + 1) * HD], preferred_element_type=jnp.float32
        )


def attend_kernel(
    turn, at_ref, qs_ref, info_ref, k0, k1, k2, k3, k4, k5, v0, v1, v2, v3, v4, v5, out_ref
):
    me = at_ref[0]
    even = lax.rem(me, 2) == 0
    rows = k0.shape[0]
    slot_count = out_ref.shape[0]
    count = info_ref.shape[0] // slot_count
    here = pl.ds(pl.multiple_of(lax.rem(me + turn, count) * slot_count, slot_count), slot_count)
    group = HEADS // KVH
    lo = info_ref[here, 0:1]
    hi = info_ref[here, 1:2]
    bases = (me - 4, jnp.where(even, me - 3, me - 1), me - 2, jnp.where(even, me - 1, me - 3), me)
    biases = []
    for base in bases:
        key_pos = base * rows + lax.broadcasted_iota(jnp.int32, (slot_count, rows), 1)
        biases.append(jnp.where((key_pos >= lo) & (key_pos <= hi), 0.0, masked_score))
    bias = jnp.concatenate(biases, axis=1)[None]
    keep = (hi >= 0).astype(jnp.float32)[None]
    scale = math.log2(math.e) / math.sqrt(HD)
    for g in range(KVH):
        cols = slice(g * HD, (g + 1) * HD)
        kx = jnp.where(even, k5[:, cols], k1[:, cols])
        vx = jnp.where(even, v5[:, cols], v1[:, cols])
        kc = jnp.concatenate([k4[:, cols], kx, k2[:, cols], k3[:, cols], k0[:, cols]], axis=0)
        vc = jnp.concatenate([v4[:, cols], vx, v2[:, cols], v3[:, cols], v0[:, cols]], axis=0)
        q = qs_ref[g * group : (g + 1) * group, here]
        q = q.reshape(group * slot_count, HD).astype(jnp.bfloat16)
        s = lax.dot_general(q, kc, (((1,), (1,)), ((), ())), preferred_element_type=jnp.float32)
        s = s.reshape(group, slot_count, s.shape[1]) * scale + bias
        p = jnp.exp2(s - jnp.max(s, axis=2, keepdims=True))
        p = p * (keep / jnp.sum(p, axis=2, keepdims=True))
        p = p.astype(jnp.bfloat16).reshape(group * slot_count, p.shape[2])
        o = jnp.dot(p, vc, preferred_element_type=jnp.float32)
        for h in range(group):
            head = g * group + h
            out_ref[:, head * HD : (head + 1) * HD] = o[
                h * slot_count : (h + 1) * slot_count
            ].astype(jnp.bfloat16)


def lay_kernel(turns, at_ref, *refs):
    count = len(turns)
    blocks, out_ref, sems = refs[:count], refs[count], refs[count + 1]
    me = at_ref[0]
    ctx_count = out_ref.shape[0]
    copies = []
    for n, turn in enumerate(turns):
        source = lax.rem(me + ctx_count - turn, ctx_count)
        copies.append(pltpu.make_async_copy(blocks[n], out_ref.at[source], sems.at[n]))
    for copy in copies:
        copy.start()
    for copy in copies:
        copy.wait()


def vmem():
    return pl.BlockSpec(memory_space=VM)


def smem():
    return pl.BlockSpec(memory_space=pltpu.SMEM)


def body(queries, keys, values, doc_lengths, row_owner):
    rows = queries.shape[0]
    count = lax.axis_size("ctx")
    slot_count = max(3, 3 * rows // (2 * count))
    if count % 2 or count > 16 or slot_count % 8 or rows % 128 or rows != keys.shape[0]:
        return plain_body(queries, keys, values, doc_lengths, row_owner, slot_count)
    me = lax.axis_index("ctx")
    slots = count * slot_count
    width = HEADS * HD

    up = [(i, i + 2) for i in range(count - 2)]
    swap = [(i, i ^ 1) for i in range(count)]
    near_k = lax.ppermute(keys, "ctx", up)
    near_v = lax.ppermute(values, "ctx", up)
    side_k = lax.ppermute(keys, "ctx", swap)
    side_v = lax.ppermute(values, "ctx", swap)
    at = jnp.full((1,), me, jnp.int32)
    qs, info = pl.pallas_call(
        functools.partial(order_kernel, count, slot_count),
        out_shape=(
            jax.ShapeDtypeStruct((HEADS, slots, HD), jnp.float32),
            jax.ShapeDtypeStruct((slots, INFO), jnp.int32),
        ),
        in_specs=[smem(), smem(), vmem(), vmem()],
        out_specs=(vmem(), vmem()),
        cost_estimate=pl.CostEstimate(
            flops=2 * slots * rows * width, bytes_accessed=5 * slots * width, transcendentals=0
        ),
        name="order",
        compiler_params=pltpu.CompilerParams(vmem_limit_bytes=GRANT),
    )(at, doc_lengths, row_owner.reshape(1, rows), queries)

    near_k, near_v, info = lax.optimization_barrier((near_k, near_v, info))
    far_k = lax.ppermute(near_k, "ctx", up)
    near_side_k = lax.ppermute(near_k, "ctx", swap)
    far_v = lax.ppermute(near_v, "ctx", up)
    near_side_v = lax.ppermute(near_v, "ctx", swap)
    far_side_k = lax.ppermute(far_k, "ctx", swap)
    far_side_v = lax.ppermute(far_v, "ctx", swap)

    key_blocks = (keys, side_k, near_k, near_side_k, far_k, far_side_k)
    value_blocks = (values, side_v, near_v, near_side_v, far_v, far_side_v)

    def attend(turn):
        return pl.pallas_call(
            functools.partial(attend_kernel, turn),
            out_shape=jax.ShapeDtypeStruct((slot_count, width), jnp.bfloat16),
            in_specs=[smem()] + [vmem()] * 14,
            out_specs=vmem(),
            cost_estimate=pl.CostEstimate(
                flops=4 * slot_count * width * 5 * rows,
                bytes_accessed=12 * rows * KVH * HD * 2 + 6 * slot_count * width,
                transcendentals=slot_count * HEADS * 5 * rows,
            ),
            compiler_params=pltpu.CompilerParams(vmem_limit_bytes=GRANT),
            name="attend",
        )(at, qs, info, *key_blocks, *value_blocks)

    half = count // 2
    turns = [half]
    for step in range(1, half):
        turns += [half - step, half + step]
    blocks = []
    for turn in turns:
        block = attend(turn)
        blocks.append(lax.ppermute(block, "ctx", [(i, (i + turn) % count) for i in range(count)]))
    blocks.append(attend(0))
    turns.append(0)

    handed = pl.pallas_call(
        functools.partial(lay_kernel, tuple(turns)),
        out_shape=jax.ShapeDtypeStruct((count, slot_count, width), jnp.bfloat16),
        in_specs=[smem()] + [vmem()] * count,
        out_specs=pl.BlockSpec(memory_space=pl.ANY),
        scratch_shapes=[pltpu.SemaphoreType.DMA((count,))],
        cost_estimate=pl.CostEstimate(
            flops=0, bytes_accessed=4 * slots * width, transcendentals=0
        ),
        name="lay",
        compiler_params=pltpu.CompilerParams(vmem_limit_bytes=GRANT),
    )(at, *blocks)
    return handed.reshape(slots, width)


def solution(mesh):
    placed = (
        P(("dp", "ctx"), None),
        P(("dp", "ctx"), None),
        P(("dp", "ctx"), None),
        P("dp"),
        P(("dp", "ctx"), None),
    )
    return jax.shard_map(
        body, mesh=mesh, in_specs=placed, out_specs=P(("dp", "ctx"), None), check_vma=False
    )
```

```python
import functools
import math

import jax
import jax.numpy as jnp
from jax import lax
from jax.experimental import pallas as pl
from jax.experimental.pallas import tpu as pltpu
from jax.sharding import PartitionSpec as P

HEADS = 32
KVH = 4
HD = 128
WIN_DEV = 4

masked_score = -1e30


def shifted(block, axis, distance):
    devices = range(lax.axis_size(axis))
    route = [(i - distance, i) for i in devices if i - distance in devices]
    return lax.ppermute(block, axis, route)


def block_scores(grouped, key_part, allowed_part):
    key_heads = key_part.reshape(key_part.shape[0], grouped.shape[1], HD)
    scores = jnp.einsum(
        "tkgd,skd->kgts", grouped, key_heads, preferred_element_type=jnp.float32
    ) * (1.0 / math.sqrt(HD))
    return jnp.where(allowed_part[None, None], scores, masked_score)


def softmax_weights(scores):
    peak = jnp.max(scores, axis=-1, keepdims=True)
    weights = jnp.exp(scores - peak)
    total = jnp.sum(weights, axis=-1, keepdims=True)
    return (weights / total).astype(jnp.bfloat16)


def mix_block(probs_part, value_part):
    value_heads = value_part.reshape(value_part.shape[0], probs_part.shape[0], HD)
    return jnp.einsum("kgts,skd->tkgd", probs_part, value_heads, preferred_element_type=jnp.float32)


def doc_numbers(doc_ends, positions):
    return jnp.sum((doc_ends[None, :] <= positions[:, None]).astype(jnp.int32), axis=1)


def plain_body(queries, keys, values, doc_lengths, row_owner, slot_count):
    row_count = queries.shape[0]
    ctx_count = lax.axis_size("ctx")
    device_index = lax.axis_index("ctx")
    group_size = HEADS // KVH
    stack_keys, stack_values = (keys, values)
    reach_width = 1
    for _ in range(WIN_DEV.bit_length() - 1):
        moved_keys, moved_values = shifted((stack_keys, stack_values), "ctx", reach_width)
        stack_keys = jnp.concatenate([moved_keys, stack_keys], axis=0)
        stack_values = jnp.concatenate([moved_values, stack_values], axis=0)
        reach_width = reach_width * 2
    far_keys, far_values = shifted((keys, values), "ctx", WIN_DEV)
    window_keys = jnp.concatenate([far_keys, stack_keys], axis=0)
    window_values = jnp.concatenate([far_values, stack_values], axis=0)
    query_pos = device_index * row_count + lax.iota(jnp.int32, row_count)
    key_pos = (device_index - WIN_DEV) * row_count + lax.iota(jnp.int32, (WIN_DEV + 1) * row_count)
    doc_ends = jnp.cumsum(doc_lengths)
    query_doc = doc_numbers(doc_ends, query_pos)
    key_doc = doc_numbers(doc_ends, key_pos)
    allowed = (
        (query_doc[:, None] == key_doc[None, :])
        & (key_pos[None, :] <= query_pos[:, None])
        & (key_pos[None, :] >= 0)
    )
    grouped_all = queries.reshape(row_count, KVH, group_size, HD)
    owner_column = row_owner[:, 0]
    onehot = (owner_column[:, None] == lax.iota(jnp.int32, ctx_count)[None, :]).astype(jnp.int32)
    earlier_count = jnp.cumsum(onehot, axis=0) - onehot
    slot_rank = jnp.sum(earlier_count * onehot, axis=1)
    slot_index = owner_column * slot_count + slot_rank
    probs = softmax_weights(block_scores(grouped_all, window_keys, allowed))
    attended = mix_block(probs, window_values)
    merged = attended.reshape(row_count, HEADS * HD).astype(jnp.bfloat16)
    return lax.all_to_all(
        jnp.zeros((ctx_count * slot_count, merged.shape[1]), jnp.bfloat16)
        .at[slot_index]
        .set(merged),
        "ctx",
        split_axis=0,
        concat_axis=0,
        tiled=True,
    )


VM = pltpu.VMEM
INFO = 128
GRANT = 16 * 1024 * 1024
SPLIT = (2, 2)
DIRECT = "ab"


def pack_kernel(k_ref, v_ref, *refs):
    parts, sems = refs[:-1], refs[-1]
    copies = []
    low = 0
    for part in parts:
        wide = part.shape[1] // 2
        for n, ref in enumerate((k_ref, v_ref)):
            copies.append(
                pltpu.make_async_copy(
                    ref.at[:, low : low + wide],
                    part.at[:, n * wide : (n + 1) * wide],
                    sems.at[len(copies)],
                )
            )
        low += wide
    for copy in copies:
        copy.start()
    for copy in copies:
        copy.wait()


def order_kernel(
    slot_count,
    at_ref,
    doc_ref,
    owner_ref,
    q_ref,
    other_owner_ref,
    other_q_ref,
    qs_ref,
    info_ref,
    docs,
    owners,
    q_in,
    sems,
):
    pieces = q_in.shape[0]
    wide = q_in.shape[2]
    doc_copy = pltpu.make_async_copy(doc_ref, docs, sems.at[pieces])
    owner_copy = pltpu.make_async_copy(owner_ref, owners, sems.at[pieces + 1])
    q_copies = [
        pltpu.make_async_copy(q_ref.at[:, n * wide : (n + 1) * wide], q_in.at[n], sems.at[n])
        for n in range(pieces)
    ]
    doc_copy.start()
    owner_copy.start()
    for copy in q_copies:
        copy.start()
    doc_copy.wait()
    owner_copy.wait()
    rows = owners.shape[1]
    slots = info_ref.shape[0]
    ctx_count = slots // slot_count
    me = at_ref[0]
    core = lax.rem(me, 2)
    upper = (
        lax.broadcasted_iota(jnp.int32, (rows, rows), 0)
        < lax.broadcasted_iota(jnp.int32, (rows, rows), 1)
    ).astype(jnp.bfloat16)
    slot = lax.broadcasted_iota(jnp.int32, (slots, rows), 0)
    place = lax.broadcasted_iota(jnp.int32, (slots, rows), 1)
    picks, pos = [], None
    for owner, source in ((owners[...], core), (other_owner_ref[...], 1 - core)):
        named = lax.broadcasted_iota(jnp.int32, (ctx_count, rows), 0) == owner
        onehot = named.astype(jnp.float32)
        earlier = jnp.dot(onehot.astype(jnp.bfloat16), upper, preferred_element_type=jnp.float32)
        rank = jnp.sum(earlier * onehot, axis=0, keepdims=True).astype(jnp.int32)
        target = ((owner // 2) * 2 + source) * slot_count + rank
        pick = slot == jnp.where(lax.rem(owner, 2) == core, target, -1)
        base = (me - core + source) * rows
        found = jnp.max(jnp.where(pick, place + base, -1), axis=1, keepdims=True)
        pos = found if pos is None else jnp.maximum(pos, found)
        picks.append(jnp.where(pick, 1.0, 0.0).astype(jnp.bfloat16))
    start = jnp.zeros_like(pos)
    end = jnp.int32(0)
    for c in range(docs.shape[0]):
        end = end + docs[c]
        start = jnp.where(end <= pos, jnp.maximum(start, end), start)
    lane = lax.broadcasted_iota(jnp.int32, (slots, INFO), 1)
    info_ref[...] = jnp.where(lane == 0, start, pos)
    pick = jnp.concatenate(picks, axis=1)
    for n in range(pieces):
        q_copies[n].wait()
        for h in range(0, wide // HD, 2):
            head = n * (wide // HD) + h
            q = jnp.concatenate(
                [
                    q_in[n, :, h * HD : (h + 2) * HD],
                    other_q_ref[:, head * HD : (head + 2) * HD],
                ],
                axis=0,
            )
            q = jnp.dot(pick, q, preferred_element_type=jnp.float32)
            qs_ref[head] = q[:, :HD]
            qs_ref[head + 1] = q[:, HD:]


def attend_kernel(shift, first_head, heads, at_ref, qs_ref, info_ref, *refs):
    out_ref = refs[-1]
    me = at_ref[0]
    other = me + 1 - 2 * lax.rem(me, 2)
    rows = refs[0].shape[0]
    slot_count = out_ref.shape[0]
    chips = info_ref.shape[0] // slot_count
    here = lax.rem(me // 2 + shift, chips) * slot_count
    here = pl.ds(pl.multiple_of(here, slot_count), slot_count)
    group = HEADS // KVH
    lo = info_ref[here, 0:1]
    hi = info_ref[here, 1:2]
    biases = []
    for base in (me, other, me - 2, other - 2, me - 4, other - 4):
        key_pos = base * rows + lax.broadcasted_iota(jnp.int32, (slot_count, rows), 1)
        biases.append(jnp.where((key_pos >= lo) & (key_pos <= hi), 0.0, masked_score))
    bias = jnp.concatenate(biases, axis=1)[None]
    keep = (hi >= 0).astype(jnp.float32)[None]
    scale = math.log2(math.e) / math.sqrt(HD)
    for n, (part, place, share) in enumerate(heads):
        blocks = refs[6 * part : 6 * part + 6]
        kc = jnp.concatenate([b[:, place * HD : (place + 1) * HD] for b in blocks], axis=0)
        place += share
        vc = jnp.concatenate([b[:, place * HD : (place + 1) * HD] for b in blocks], axis=0)
        first = (first_head + n) * group
        q = qs_ref[first : first + group, here]
        q = q.reshape(group * slot_count, HD).astype(jnp.bfloat16)
        s = lax.dot_general(q, kc, (((1,), (1,)), ((), ())), preferred_element_type=jnp.float32)
        s = s.reshape(group, slot_count, s.shape[1]) * scale + bias
        p = jnp.exp2(s - jnp.max(s, axis=2, keepdims=True))
        p = p * (keep / jnp.sum(p, axis=2, keepdims=True))
        p = p.astype(jnp.bfloat16).reshape(group * slot_count, p.shape[2])
        o = jnp.dot(p, vc, preferred_element_type=jnp.float32)
        for h in range(group):
            at = (n * group + h) * HD
            out_ref[:, at : at + HD] = o[h * slot_count : (h + 1) * slot_count].astype(jnp.bfloat16)


def lay_kernel(places, at_ref, *refs):
    total = len(places)
    blocks, out_ref, sems = refs[:total], refs[total], refs[total + 1]
    chip = at_ref[0] // 2
    chips = out_ref.shape[0]
    copies = []
    for n, (shift, at) in enumerate(places):
        source = lax.rem(chip + chips - shift, chips)
        wide = blocks[n].shape[1]
        copies.append(
            pltpu.make_async_copy(blocks[n], out_ref.at[source, :, at : at + wide], sems.at[n])
        )
    for copy in copies:
        copy.start()
    for copy in copies:
        copy.wait()


def hbm():
    return pl.BlockSpec(memory_space=pltpu.HBM)


def vmem():
    return pl.BlockSpec(memory_space=VM)


def smem():
    return pl.BlockSpec(memory_space=pltpu.SMEM)


def hand_plan(count):
    chips = count // 2
    shifts = [chips // 2]
    for step in range(1, chips // 2):
        shifts += [chips // 2 - step, chips // 2 + step]
    if chips % 2:
        shifts.append(chips - 1)
    plan = [(shift, 0, SPLIT[0]) for shift in shifts]
    plan += [(shift, SPLIT[0], KVH) for shift in shifts]
    return plan + [(0, 0, KVH)]


def fits(count, rows):
    slot_count = max(3, 3 * rows // (2 * count))
    return count % 2 == 0 and count <= 16 and slot_count % 8 == 0 and rows % 128 == 0


def body(queries, keys, values, doc_lengths, row_owner):
    rows = queries.shape[0]
    count = lax.axis_size("ctx")
    slot_count = max(3, 3 * rows // (2 * count))
    if not fits(count, rows):
        return plain_body(queries, keys, values, doc_lengths, row_owner, slot_count)
    me = lax.axis_index("ctx")
    slots = count * slot_count
    width = HEADS * HD

    up = [(i, i + 2) for i in range(count - 2)]
    up_twice = [(i, i + 4) for i in range(count - 4)]
    swap = [(i, i ^ 1) for i in range(count)]
    at = jnp.full((1,), me, jnp.int32)
    params = pltpu.CompilerParams(vmem_limit_bytes=GRANT)

    def hop(block, route):
        return lax.ppermute(block, "ctx", route)

    packed = pl.pallas_call(
        pack_kernel,
        out_shape=[jax.ShapeDtypeStruct((rows, 2 * n * HD), jnp.bfloat16) for n in SPLIT],
        in_specs=[hbm(), hbm()],
        out_specs=[vmem() for n in SPLIT],
        scratch_shapes=[pltpu.SemaphoreType.DMA((2 * len(SPLIT),))],
        compiler_params=params,
        name="pack",
    )(*[pltpu.with_memory_space_constraint(part, pltpu.HBM) for part in (keys, values)])
    windows = []
    for own, tag in zip(packed, "ab"):
        near = hop(own, up)
        far = hop(own, up_twice) if tag in DIRECT else hop(near, up)
        windows.append((own, hop(own, swap), near, hop(near, swap), far, hop(far, swap)))

    owner_line = row_owner.reshape(1, rows)
    other_q = hop(queries, swap)
    other_owner = hop(owner_line, swap)
    pieces = 4
    order = pl.pallas_call(
        functools.partial(order_kernel, slot_count),
        out_shape=(
            jax.ShapeDtypeStruct((HEADS, slots, HD), jnp.float32),
            jax.ShapeDtypeStruct((slots, INFO), jnp.int32),
        ),
        in_specs=[smem(), hbm(), hbm(), hbm(), vmem(), vmem()],
        out_specs=(vmem(), vmem()),
        scratch_shapes=[
            pltpu.SMEM(doc_lengths.shape, jnp.int32),
            pltpu.VMEM((1, rows), jnp.int32),
            pltpu.VMEM((pieces, rows, width // pieces), jnp.bfloat16),
            pltpu.SemaphoreType.DMA((pieces + 2,)),
        ],
        cost_estimate=pl.CostEstimate(
            flops=4 * slots * rows * width, bytes_accessed=6 * slots * width, transcendentals=0
        ),
        compiler_params=params,
        name="order",
    )
    outside = [
        pltpu.with_memory_space_constraint(part, pltpu.HBM)
        for part in (doc_lengths, owner_line, queries)
    ]
    qs, info = order(at, *outside, other_owner, other_q)

    both = 2 * slot_count

    def attend(shift, low, high):
        share = (high - low) * (HEADS // KVH) * HD
        used = [n for n in range(2) if (low < SPLIT[0], high > SPLIT[0])[n]]
        heads = []
        for g in range(low, high):
            part = int(g >= SPLIT[0])
            heads.append((used.index(part), g - part * SPLIT[0], SPLIT[part]))
        blocks = sum([windows[n] for n in used], ())
        return pl.pallas_call(
            functools.partial(attend_kernel, shift, low, tuple(heads)),
            out_shape=jax.ShapeDtypeStruct((both, share), jnp.bfloat16),
            in_specs=[smem()] + [vmem()] * (2 + len(blocks)),
            out_specs=vmem(),
            cost_estimate=pl.CostEstimate(
                flops=4 * both * share * 6 * rows,
                bytes_accessed=3 * rows * share + 6 * both * share,
                transcendentals=both * share // HD * 6 * rows,
            ),
            compiler_params=params,
            name="attend",
        )(at, qs, info, *blocks)

    places, blocks = [], []
    for shift, low, high in hand_plan(count):
        block = attend(shift, low, high)
        if shift:
            route = [(i, (i + 2 * shift) % count) for i in range(count)]
            block = hop(block, route)
        blocks.append(block)
        places.append((shift, low * (HEADS // KVH) * HD))

    handed = pl.pallas_call(
        functools.partial(lay_kernel, tuple(places)),
        out_shape=jax.ShapeDtypeStruct((count // 2, both, width), jnp.bfloat16),
        in_specs=[smem()] + [vmem()] * len(blocks),
        out_specs=hbm(),
        scratch_shapes=[pltpu.SemaphoreType.DMA((len(blocks),))],
        cost_estimate=pl.CostEstimate(
            flops=0, bytes_accessed=4 * slots * width, transcendentals=0
        ),
        compiler_params=params,
        name="lay",
    )(at, *blocks)
    return handed.reshape(slots, width)


def solution(mesh):
    placed = (
        P(("dp", "ctx"), None),
        P(("dp", "ctx"), None),
        P(("dp", "ctx"), None),
        P("dp"),
        P(("dp", "ctx"), None),
    )

    return jax.shard_map(
        body, mesh=mesh, in_specs=placed, out_specs=P(("dp", "ctx"), None), check_vma=False
    )
```

```python
import functools
import math

import jax
import jax.numpy as jnp
from jax import lax
from jax.experimental import pallas as pl
from jax.experimental.pallas import tpu as pltpu
from jax.sharding import PartitionSpec as P

HEADS = 32
KVH = 4
HD = 128
WIN_DEV = 4

masked_score = -1e30


def shifted(block, axis, distance):
    devices = range(lax.axis_size(axis))
    route = [(i - distance, i) for i in devices if i - distance in devices]
    return lax.ppermute(block, axis, route)


def block_scores(grouped, key_part, allowed_part):
    key_heads = key_part.reshape(key_part.shape[0], grouped.shape[1], HD)
    scores = jnp.einsum(
        "tkgd,skd->kgts", grouped, key_heads, preferred_element_type=jnp.float32
    ) * (1.0 / math.sqrt(HD))
    return jnp.where(allowed_part[None, None], scores, masked_score)


def softmax_weights(scores):
    peak = jnp.max(scores, axis=-1, keepdims=True)
    weights = jnp.exp(scores - peak)
    total = jnp.sum(weights, axis=-1, keepdims=True)
    return (weights / total).astype(jnp.bfloat16)


def mix_block(probs_part, value_part):
    value_heads = value_part.reshape(value_part.shape[0], probs_part.shape[0], HD)
    return jnp.einsum("kgts,skd->tkgd", probs_part, value_heads, preferred_element_type=jnp.float32)


def doc_numbers(doc_ends, positions):
    return jnp.sum((doc_ends[None, :] <= positions[:, None]).astype(jnp.int32), axis=1)


def plain_body(queries, keys, values, doc_lengths, row_owner, slot_count):
    row_count = queries.shape[0]
    ctx_count = lax.axis_size("ctx")
    device_index = lax.axis_index("ctx")
    group_size = HEADS // KVH
    stack_keys, stack_values = (keys, values)
    reach_width = 1
    for _ in range(WIN_DEV.bit_length() - 1):
        moved_keys, moved_values = shifted((stack_keys, stack_values), "ctx", reach_width)
        stack_keys = jnp.concatenate([moved_keys, stack_keys], axis=0)
        stack_values = jnp.concatenate([moved_values, stack_values], axis=0)
        reach_width = reach_width * 2
    far_keys, far_values = shifted((keys, values), "ctx", WIN_DEV)
    window_keys = jnp.concatenate([far_keys, stack_keys], axis=0)
    window_values = jnp.concatenate([far_values, stack_values], axis=0)
    query_pos = device_index * row_count + lax.iota(jnp.int32, row_count)
    key_pos = (device_index - WIN_DEV) * row_count + lax.iota(jnp.int32, (WIN_DEV + 1) * row_count)
    doc_ends = jnp.cumsum(doc_lengths)
    query_doc = doc_numbers(doc_ends, query_pos)
    key_doc = doc_numbers(doc_ends, key_pos)
    allowed = (
        (query_doc[:, None] == key_doc[None, :])
        & (key_pos[None, :] <= query_pos[:, None])
        & (key_pos[None, :] >= 0)
    )
    grouped_all = queries.reshape(row_count, KVH, group_size, HD)
    owner_column = row_owner[:, 0]
    onehot = (owner_column[:, None] == lax.iota(jnp.int32, ctx_count)[None, :]).astype(jnp.int32)
    earlier_count = jnp.cumsum(onehot, axis=0) - onehot
    slot_rank = jnp.sum(earlier_count * onehot, axis=1)
    slot_index = owner_column * slot_count + slot_rank
    probs = softmax_weights(block_scores(grouped_all, window_keys, allowed))
    attended = mix_block(probs, window_values)
    merged = attended.reshape(row_count, HEADS * HD).astype(jnp.bfloat16)
    return lax.all_to_all(
        jnp.zeros((ctx_count * slot_count, merged.shape[1]), jnp.bfloat16)
        .at[slot_index]
        .set(merged),
        "ctx",
        split_axis=0,
        concat_axis=0,
        tiled=True,
    )


VM = pltpu.VMEM
INFO = 128
GRANT = 16 * 1024 * 1024
SPLIT = (2, 2)
DIRECT = "ab"


def pack_kernel(k_ref, v_ref, *refs):
    parts, sems = refs[:-1], refs[-1]
    copies = []
    low = 0
    for part in parts:
        wide = part.shape[1] // 2
        for n, ref in enumerate((k_ref, v_ref)):
            copies.append(
                pltpu.make_async_copy(
                    ref.at[:, low : low + wide],
                    part.at[:, n * wide : (n + 1) * wide],
                    sems.at[len(copies)],
                )
            )
        low += wide
    for copy in copies:
        copy.start()
    for copy in copies:
        copy.wait()


def order_kernel(
    slot_count,
    at_ref,
    doc_ref,
    owner_ref,
    q_ref,
    other_owner_ref,
    other_q_ref,
    qs_ref,
    info_ref,
    docs,
    owners,
    q_in,
    sems,
):
    pieces = q_in.shape[0]
    wide = q_in.shape[2]
    doc_copy = pltpu.make_async_copy(doc_ref, docs, sems.at[pieces])
    owner_copy = pltpu.make_async_copy(owner_ref, owners, sems.at[pieces + 1])
    q_copies = [
        pltpu.make_async_copy(q_ref.at[:, n * wide : (n + 1) * wide], q_in.at[n], sems.at[n])
        for n in range(pieces)
    ]
    doc_copy.start()
    owner_copy.start()
    for copy in q_copies:
        copy.start()
    doc_copy.wait()
    owner_copy.wait()
    rows = owners.shape[1]
    slots = info_ref.shape[0]
    ctx_count = slots // slot_count
    me = at_ref[0]
    core = lax.rem(me, 2)
    upper = (
        lax.broadcasted_iota(jnp.int32, (rows, rows), 0)
        < lax.broadcasted_iota(jnp.int32, (rows, rows), 1)
    ).astype(jnp.bfloat16)
    slot = lax.broadcasted_iota(jnp.int32, (slots, rows), 0)
    place = lax.broadcasted_iota(jnp.int32, (slots, rows), 1)
    picks, pos = [], None
    for owner, source in ((owners[...], core), (other_owner_ref[...], 1 - core)):
        named = lax.broadcasted_iota(jnp.int32, (ctx_count, rows), 0) == owner
        onehot = named.astype(jnp.float32)
        earlier = jnp.dot(onehot.astype(jnp.bfloat16), upper, preferred_element_type=jnp.float32)
        rank = jnp.sum(earlier * onehot, axis=0, keepdims=True).astype(jnp.int32)
        target = ((owner // 2) * 2 + source) * slot_count + rank
        pick = slot == jnp.where(lax.rem(owner, 2) == core, target, -1)
        base = (me - core + source) * rows
        found = jnp.max(jnp.where(pick, place + base, -1), axis=1, keepdims=True)
        pos = found if pos is None else jnp.maximum(pos, found)
        picks.append(jnp.where(pick, 1.0, 0.0).astype(jnp.bfloat16))
    start = jnp.zeros_like(pos)
    end = jnp.int32(0)
    for c in range(docs.shape[0]):
        end = end + docs[c]
        start = jnp.where(end <= pos, jnp.maximum(start, end), start)
    lane = lax.broadcasted_iota(jnp.int32, (slots, INFO), 1)
    info_ref[...] = jnp.where(lane == 0, start, pos)
    pick = jnp.concatenate(picks, axis=1)
    for n in range(pieces):
        q_copies[n].wait()
        for h in range(0, wide // HD, 2):
            head = n * (wide // HD) + h
            q = jnp.concatenate(
                [
                    q_in[n, :, h * HD : (h + 2) * HD],
                    other_q_ref[:, head * HD : (head + 2) * HD],
                ],
                axis=0,
            )
            q = jnp.dot(pick, q, preferred_element_type=jnp.float32)
            qs_ref[head] = q[:, :HD]
            qs_ref[head + 1] = q[:, HD:]


def attend_kernel(shift, first_head, heads, at_ref, qs_ref, info_ref, *refs):
    out_ref = refs[-1]
    me = at_ref[0]
    other = me + 1 - 2 * lax.rem(me, 2)
    rows = refs[0].shape[0]
    slot_count = out_ref.shape[0]
    chips = info_ref.shape[0] // slot_count
    here = lax.rem(me // 2 + shift, chips) * slot_count
    here = pl.ds(pl.multiple_of(here, slot_count), slot_count)
    group = HEADS // KVH
    lo = info_ref[here, 0:1]
    hi = info_ref[here, 1:2]
    biases = []
    for base in (me, other, me - 2, other - 2, me - 4, other - 4):
        key_pos = base * rows + lax.broadcasted_iota(jnp.int32, (slot_count, rows), 1)
        biases.append(jnp.where((key_pos >= lo) & (key_pos <= hi), 0.0, masked_score))
    bias = jnp.concatenate(biases, axis=1)[None]
    keep = (hi >= 0).astype(jnp.float32)[None]
    scale = math.log2(math.e) / math.sqrt(HD)
    for n, (part, place, share) in enumerate(heads):
        blocks = refs[6 * part : 6 * part + 6]
        kc = jnp.concatenate([b[:, place * HD : (place + 1) * HD] for b in blocks], axis=0)
        place += share
        vc = jnp.concatenate([b[:, place * HD : (place + 1) * HD] for b in blocks], axis=0)
        first = (first_head + n) * group
        q = qs_ref[first : first + group, here]
        q = q.reshape(group * slot_count, HD).astype(jnp.bfloat16)
        s = lax.dot_general(q, kc, (((1,), (1,)), ((), ())), preferred_element_type=jnp.float32)
        s = s.reshape(group, slot_count, s.shape[1]) * scale + bias
        p = jnp.exp2(s - jnp.max(s, axis=2, keepdims=True))
        p = p * (keep / jnp.sum(p, axis=2, keepdims=True))
        p = p.astype(jnp.bfloat16).reshape(group * slot_count, p.shape[2])
        o = jnp.dot(p, vc, preferred_element_type=jnp.float32)
        for h in range(group):
            at = (n * group + h) * HD
            out_ref[:, at : at + HD] = o[h * slot_count : (h + 1) * slot_count].astype(jnp.bfloat16)


def lay_kernel(places, onto, at_ref, *refs):
    total = len(places)
    blocks, out_ref, sems = refs[:total], refs[total + onto], refs[total + onto + 1]
    chip = at_ref[0] // 2
    chips = out_ref.shape[0]
    copies = []
    for n, (shift, at) in enumerate(places):
        source = lax.rem(chip + chips - shift, chips)
        wide = blocks[n].shape[1]
        copies.append(
            pltpu.make_async_copy(blocks[n], out_ref.at[source, :, at : at + wide], sems.at[n])
        )
    for copy in copies:
        copy.start()
    for copy in copies:
        copy.wait()


def hbm():
    return pl.BlockSpec(memory_space=pltpu.HBM)


def vmem():
    return pl.BlockSpec(memory_space=VM)


def smem():
    return pl.BlockSpec(memory_space=pltpu.SMEM)


def hand_plan(count):
    chips = count // 2
    shifts = [chips // 2]
    for step in range(1, chips // 2):
        shifts += [chips // 2 - step, chips // 2 + step]
    if chips % 2:
        shifts.append(chips - 1)
    plan = [(shift, 0, SPLIT[0]) for shift in shifts]
    plan += [(shift, SPLIT[0], KVH) for shift in shifts]
    return plan + [(0, 0, KVH)]


def fits(count, rows):
    slot_count = max(3, 3 * rows // (2 * count))
    return count % 2 == 0 and count <= 16 and slot_count % 8 == 0 and rows % 128 == 0


def body(queries, keys, values, doc_lengths, row_owner):
    rows = queries.shape[0]
    count = lax.axis_size("ctx")
    slot_count = max(3, 3 * rows // (2 * count))
    if not fits(count, rows):
        return plain_body(queries, keys, values, doc_lengths, row_owner, slot_count)
    me = lax.axis_index("ctx")
    slots = count * slot_count
    width = HEADS * HD

    up = [(i, i + 2) for i in range(count - 2)]
    up_twice = [(i, i + 4) for i in range(count - 4)]
    swap = [(i, i ^ 1) for i in range(count)]
    at = jnp.full((1,), me, jnp.int32)
    params = pltpu.CompilerParams(vmem_limit_bytes=GRANT)

    def hop(block, route):
        return lax.ppermute(block, "ctx", route)

    packed = pl.pallas_call(
        pack_kernel,
        out_shape=[jax.ShapeDtypeStruct((rows, 2 * n * HD), jnp.bfloat16) for n in SPLIT],
        in_specs=[hbm(), hbm()],
        out_specs=[vmem() for n in SPLIT],
        scratch_shapes=[pltpu.SemaphoreType.DMA((2 * len(SPLIT),))],
        compiler_params=params,
        name="pack",
    )(*[pltpu.with_memory_space_constraint(part, pltpu.HBM) for part in (keys, values)])
    windows = []
    for own, tag in zip(packed, "ab"):
        near = hop(own, up)
        far = hop(own, up_twice) if tag in DIRECT else hop(near, up)
        windows.append((own, hop(own, swap), near, hop(near, swap), far, hop(far, swap)))

    owner_line = row_owner.reshape(1, rows)
    other_q = hop(queries, swap)
    other_owner = hop(owner_line, swap)
    pieces = 4
    order = pl.pallas_call(
        functools.partial(order_kernel, slot_count),
        out_shape=(
            jax.ShapeDtypeStruct((HEADS, slots, HD), jnp.float32),
            jax.ShapeDtypeStruct((slots, INFO), jnp.int32),
        ),
        in_specs=[smem(), hbm(), hbm(), hbm(), vmem(), vmem()],
        out_specs=(vmem(), vmem()),
        scratch_shapes=[
            pltpu.SMEM(doc_lengths.shape, jnp.int32),
            pltpu.VMEM((1, rows), jnp.int32),
            pltpu.VMEM((pieces, rows, width // pieces), jnp.bfloat16),
            pltpu.SemaphoreType.DMA((pieces + 2,)),
        ],
        cost_estimate=pl.CostEstimate(
            flops=4 * slots * rows * width, bytes_accessed=6 * slots * width, transcendentals=0
        ),
        compiler_params=params,
        name="order",
    )
    outside = [
        pltpu.with_memory_space_constraint(part, pltpu.HBM)
        for part in (doc_lengths, owner_line, queries)
    ]
    qs, info = order(at, *outside, other_owner, other_q)

    both = 2 * slot_count

    def attend(shift, low, high):
        share = (high - low) * (HEADS // KVH) * HD
        used = [n for n in range(2) if (low < SPLIT[0], high > SPLIT[0])[n]]
        heads = []
        for g in range(low, high):
            part = int(g >= SPLIT[0])
            heads.append((used.index(part), g - part * SPLIT[0], SPLIT[part]))
        blocks = sum([windows[n] for n in used], ())
        return pl.pallas_call(
            functools.partial(attend_kernel, shift, low, tuple(heads)),
            out_shape=jax.ShapeDtypeStruct((both, share), jnp.bfloat16),
            in_specs=[smem()] + [vmem()] * (2 + len(blocks)),
            out_specs=vmem(),
            cost_estimate=pl.CostEstimate(
                flops=4 * both * share * 6 * rows,
                bytes_accessed=3 * rows * share + 6 * both * share,
                transcendentals=both * share // HD * 6 * rows,
            ),
            compiler_params=params,
            name="attend",
        )(at, qs, info, *blocks)

    places, blocks = [], []
    for shift, low, high in hand_plan(count):
        block = attend(shift, low, high)
        if shift:
            route = [(i, (i + 2 * shift) % count) for i in range(count)]
            block = hop(block, route)
        blocks.append(block)
        places.append((shift, low * (HEADS // KVH) * HD))

    shape = jax.ShapeDtypeStruct((count // 2, both, width), jnp.bfloat16)

    def lay(picked, handed):
        chosen = [blocks[n] for n in picked]
        return pl.pallas_call(
            functools.partial(lay_kernel, tuple(places[n] for n in picked), handed is not None),
            out_shape=shape,
            in_specs=[smem()] + [vmem()] * len(chosen) + [hbm()] * (handed is not None),
            out_specs=hbm(),
            scratch_shapes=[pltpu.SemaphoreType.DMA((len(chosen),))],
            input_output_aliases={1 + len(chosen): 0} if handed is not None else {},
            cost_estimate=pl.CostEstimate(
                flops=0, bytes_accessed=4 * slots * width, transcendentals=0
            ),
            compiler_params=params,
            name="lay",
        )(at, *chosen, *([handed] if handed is not None else []))

    sends = len(blocks) - 1
    handed = lay(list(range(sends - 2)) + [sends], None)
    handed = lay(list(range(sends - 2, sends)), handed)
    return handed.reshape(slots, width)


def solution(mesh):
    placed = (
        P(("dp", "ctx"), None),
        P(("dp", "ctx"), None),
        P(("dp", "ctx"), None),
        P("dp"),
        P(("dp", "ctx"), None),
    )

    return jax.shard_map(
        body, mesh=mesh, in_specs=placed, out_specs=P(("dp", "ctx"), None), check_vma=False
    )
```
